8 devices in a mesh: dp: 1 (over z), ep: 8 (over x, y, core).
Axes of the slice: x: 2, y: 2, z: 1, core: 2. Of those that a mesh axis runs over, the one named last changes fastest.
Arguments:
- x: bfloat16 [1, 8, 256, 2048], P('dp', 'ep')
- expert: int32 [1, 8, 256, 8], P('dp', 'ep')
- slot: int32 [1, 8, 256, 8], P('dp', 'ep')
- gate: float32 [1, 8, 256, 8], P('dp', 'ep')
- w_gate: bfloat16 [64, 2048, 1024], P('ep')
- w_up: bfloat16 [64, 2048, 1024], P('ep')
- w_down: bfloat16 [64, 1024, 2048], P('ep')
Outputs:
- y: bfloat16 [1, 8, 256, 2048], P('dp', 'ep')
All inputs are finite; a program needn't handle non-finite values.
Results may differ from the reference program's by a relative error of at most 0.009.
Values are sent between devices in bfloat16 or wider.
A program may use at most 2 GiB of HBM per device.

```python
import jax
import jax.numpy as jnp

MEMBERS = 8
TOKENS = 256
D = 2048
FF = 1024
TOP = 8
EXPERTS = 64
SLOTS = 5 * TOKENS * TOP // (4 * EXPERTS)


def setup_inputs(seed: int = 0, part: int = 0) -> dict:
    own, k1, k2, k3, k4, k5, k6 = jax.random.split(jax.random.key(seed), 7)
    kx, ke, kl, kg = jax.random.split(jax.random.fold_in(own, part), 4)
    devices = (1, MEMBERS)
    place = jax.random.permutation(kl, jnp.arange(EXPERTS, dtype=jnp.uint32))
    slow = ((EXPERTS + (9 * place) % EXPERTS) << ((9 * place) // EXPERTS)) // EXPERTS
    wait = (jax.random.bits(ke, (*devices, TOKENS, EXPERTS), jnp.uint32) >> 10) * slow
    expert = jnp.argsort(wait, axis=-1)[..., :TOP].astype(jnp.int32)
    chosen = jax.nn.one_hot(expert, EXPERTS, dtype=jnp.int32)
    in_line = jnp.cumsum(chosen.reshape(*devices, TOKENS * TOP, EXPERTS), axis=2) - 1
    slot = jnp.sum(in_line.reshape(chosen.shape) * chosen, axis=-1)

    def one(key, rows, columns):
        return (jax.random.normal(key, (rows, columns), jnp.float32) * rows**-0.5).astype(jnp.bfloat16)

    def weights(key, rows, columns):
        return jax.lax.map(lambda k: one(k, rows, columns), jax.random.split(key, EXPERTS))

    return {
        "x": jax.random.normal(kx, (*devices, TOKENS, D), jnp.float32).astype(jnp.bfloat16),
        "expert": expert,
        "slot": slot,
        "gate": jax.nn.softmax(jax.random.normal(kg, expert.shape, jnp.float32)),
        "w_gate": weights(k1, D, FF),
        "w_up": weights(k2, D, FF),
        "w_down": weights(k3, FF, D),
    }


def einsum(form, a, b):
    return jnp.einsum(form, a.astype(jnp.float32), b.astype(jnp.float32))


def reference(x, expert, slot, gate, w_gate, w_up, w_down):
    to_expert = jax.nn.one_hot(expert, EXPERTS, dtype=jnp.bfloat16)
    to_slot = jax.nn.one_hot(slot, SLOTS, dtype=jnp.bfloat16)
    weighted = to_expert * gate[..., None].astype(jnp.bfloat16)
    dispatch = einsum("abtke,abtkc->abtec", to_expert, to_slot).astype(jnp.bfloat16)
    combine = einsum("abtke,abtkc->abtec", weighted, to_slot).astype(jnp.bfloat16)
    z = einsum("abtec,abtd->aebcd", dispatch, x).astype(jnp.bfloat16)
    h = jax.nn.silu(einsum("aebcd,edf->aebcf", z, w_gate))
    h = (h * einsum("aebcd,edf->aebcf", z, w_up)).astype(jnp.bfloat16)
    out = einsum("aebcf,efd->aebcd", h, w_down).astype(jnp.bfloat16)
    y = einsum("abtec,aebcd->abtd", combine, out)
    return y.astype(jnp.bfloat16)
```

```python
import functools

import jax
import jax.numpy as jnp
from jax import lax
from jax.experimental import pallas as pl
from jax.experimental.pallas import tpu as pltpu
from jax.sharding import PartitionSpec as P

MESH = pl.DeviceIdType.MESH
F32, BF16 = jnp.float32, jnp.bfloat16

CORE, Y, X = 1, 2, 4
WR, DR = 6, 8
LAG = 3


def kernel(
    cfg, meta_ref, x_ref, wg_ref, wu_ref, wd_ref, o_ref,
    meta, xall, acc, hid, z, wring, dring, disp, comb, outb,
    part, psend, prec, keep, s1x, s1y, r1x, r1y, s2x, s2y, r2x, r2y,
    meta_ss, meta_rs, load_s, ag_ss, ag_rs, wsem, dsem, p_ss, p_rs, h1_ss, h1_rs, h2_ss, h2_rs,
):
    tokens, d, ff, experts, slots, kc, nc = cfg
    rows = experts * slots
    kn, nn = d // kc, d // nc
    half = tokens // 2
    wide = 2 * slots
    dp, me = lax.axis_index("dp"), lax.axis_index("ep")

    def dev(mask):
        to = me
        for bit in (CORE, Y, X):
            if mask & bit:
                to = to + bit - 2 * bit * ((me // bit) % 2)
        return (dp, to)

    def remote(src, dst, ss, rs, mask):
        return pltpu.make_async_remote_copy(
            src_ref=src, dst_ref=dst, send_sem=ss, recv_sem=rs, device_id=dev(mask), device_id_type=MESH
        )

    def w_copies(i):
        e, k, slot = i % experts, i // experts, i % WR
        at = pl.ds(pl.multiple_of(k * kc, kc), kc)
        return (
            pltpu.make_async_copy(wg_ref.at[e, at], wring.at[slot, 0], wsem.at[slot, 0]),
            pltpu.make_async_copy(wu_ref.at[e, at], wring.at[slot, 1], wsem.at[slot, 1]),
        )

    def d_copy(i):
        e, n, slot = i % experts, i // experts, i % DR
        at = pl.ds(pl.multiple_of(n * nc, nc), nc)
        return pltpu.make_async_copy(wd_ref.at[e, :, at], dring.at[slot], dsem.at[slot])

    def to_x(k):
        return remote(xall.at[0, k], xall.at[X, k], ag_ss.at[0, k], ag_rs.at[0, k], X)

    def to_y(k):
        return remote(xall.at[0, k], xall.at[Y, k], ag_ss.at[1, k], ag_rs.at[1, k], Y)

    def to_core(k):
        return remote(xall.at[0, k], xall.at[CORE, k], ag_ss.at[2, k], ag_rs.at[2, k], CORE)

    def x_to_core(k):
        return remote(xall.at[X, k], xall.at[X | CORE, k], ag_ss.at[3, k], ag_rs.at[3, k], CORE)

    def y_to_core(k):
        return remote(xall.at[Y, k], xall.at[Y | CORE, k], ag_ss.at[4, k], ag_rs.at[4, k], CORE)

    def x_to_y(k):
        at = pl.ds(0, half)
        return remote(xall.at[X, k, at], xall.at[X | Y, k, at], ag_ss.at[5, k], ag_rs.at[5, k], Y)

    def y_to_x(k):
        at = pl.ds(half, half)
        return remote(xall.at[Y, k, at], xall.at[X | Y, k, at], ag_ss.at[6, k], ag_rs.at[6, k], X)

    def xy_to_core(k):
        return remote(xall.at[X | Y, k], xall.at[7, k], ag_ss.at[7, k], ag_rs.at[7, k], CORE)

    exchange = (to_x, to_y, to_core, x_to_core, y_to_core, x_to_y, y_to_x, xy_to_core)

    def own(k):
        at = pl.ds(pl.multiple_of(k * kc, kc), kc)
        return pltpu.make_async_copy(x_ref.at[:, at], xall.at[0, k], load_s.at[k])

    for k in range(kn):
        own(k).start()
    load_meta = pltpu.make_async_copy(meta_ref, meta.at[0], load_s.at[kn])
    load_meta.start()
    for i in range(WR):
        for copy in w_copies(i):
            copy.start()

    barrier = pltpu.get_barrier_semaphore()
    for mask in range(1, 8):
        pl.semaphore_signal(barrier, inc=1, device_id=dev(mask), device_id_type=MESH)
    load_meta.wait()
    pl.semaphore_wait(barrier, 7)

    metas = [
        remote(meta.at[0], meta.at[mask], meta_ss.at[mask], meta_rs.at[mask], mask) for mask in range(1, 8)
    ]
    for copy in metas:
        copy.start()

    def first_hop(k):
        own(k).wait()
        to_x(k).start()
        to_y(k).start()
        to_core(k).start()

    first_hop(0)
    first_hop(1)

    def clear(e, _):
        acc[e] = jnp.zeros(acc.shape[1:], F32)
        return 0

    lax.fori_loop(0, experts, clear, 0)

    for copy in metas:
        copy.wait()

    def tables(r, _):
        row = lax.broadcasted_iota(jnp.int32, (rows, tokens), 0).astype(F32)
        at = meta[r]
        code = at[:8] - (me * rows).astype(F32)
        gate = at[8:]
        hit = jnp.zeros((rows, tokens), F32)
        weight = jnp.zeros((rows, tokens), F32)
        for j in range(8):
            same = code[j : j + 1] == row
            hit = jnp.where(same, 1.0, hit)
            weight = jnp.where(same, gate[j : j + 1], weight)
        disp[r] = hit.astype(BF16)
        comb[r] = jnp.transpose(weight).astype(BF16)
        return 0

    lax.fori_loop(0, 8, tables, 0)

    def project(k):
        for pair in range(4):
            z0 = jnp.dot(disp[2 * pair], xall[2 * pair, k], preferred_element_type=F32)
            z1 = jnp.dot(disp[2 * pair + 1], xall[2 * pair + 1, k], preferred_element_type=F32)
            both = jnp.concatenate(
                [z0.reshape(experts, slots, kc), z1.reshape(experts, slots, kc)], axis=1
            ).astype(BF16)
            z[:, pair * wide : (pair + 1) * wide, :] = both

        def one(e, _):
            i = k * experts + e
            slot = i % WR
            for copy in w_copies(i):
                copy.wait()
            lhs = z[e]
            step = 512
            for part_ in range(2):
                for c in range(0, ff, step):
                    got = jnp.dot(lhs, wring[slot, part_, :, c : c + step], preferred_element_type=F32)
                    acc[e, :, part_ * ff + c : part_ * ff + c + step] += got

            @pl.when(i + WR < experts * kn)
            def _():
                for copy in w_copies(i + WR):
                    copy.start()

            @pl.when(k == kn - 1)
            def _():
                for c in range(0, ff, 256):
                    g = acc[e, :, c : c + 256]
                    u = acc[e, :, ff + c : ff + c + 256]
                    hid[e, :, c : c + 256] = (g * lax.logistic(g) * u).astype(BF16)

            return 0

        lax.fori_loop(0, experts, one, 0)

    def gather_step(t, _):
        @pl.when(t < kn)
        def _():
            to_x(t).wait_recv()
            x_to_core(t).start()
            x_to_y(t).start()
            to_y(t).wait_recv()
            y_to_core(t).start()
            y_to_x(t).start()

        @pl.when(t + 2 < kn)
        def _():
            first_hop(t + 2)

        @pl.when((t >= 1) & (t < kn + 1))
        def _():
            x_to_y(t - 1).wait_recv()
            y_to_x(t - 1).wait_recv()
            xy_to_core(t - 1).start()

        @pl.when((t >= 2) & (t < kn + 2))
        def _():
            k = t - 2
            to_core(k).wait_recv()
            x_to_core(k).wait_recv()
            y_to_core(k).wait_recv()
            xy_to_core(k).wait_recv()

            @pl.when(k == kn - 1)
            def _():
                for i in range(DR):
                    d_copy(i).start()

            project(k)

        return 0

    lax.fori_loop(0, kn + 2, gather_step, 0)

    def to_part(n):
        return remote(psend.at[n % 2], prec.at[n], p_ss.at[n], p_rs.at[n], CORE)

    def hop1_x(n):
        return remote(s1x.at[n % 2], r1x.at[n], h1_ss.at[0, n], h1_rs.at[0, n], X)

    def hop1_y(n):
        return remote(s1y.at[n % 2], r1y.at[n], h1_ss.at[1, n], h1_rs.at[1, n], Y)

    def hop2_x(n):
        return remote(s2x.at[n % 2], r2x.at[n], h2_ss.at[0, n], h2_rs.at[0, n], X)

    def hop2_y(n):
        return remote(s2y.at[n % 2], r2y.at[n], h2_ss.at[1, n], h2_rs.at[1, n], Y)

    top, low = slice(0, half), slice(half, tokens)

    def reduce_step(t, _):
        @pl.when((t >= 1) & (t < nn + 1))
        def _():
            n = t - 1
            to_part(n).wait_recv()

            @pl.when(n >= 2)
            def _():
                hop1_x(n - 2).wait_send()
                hop1_y(n - 2).wait_send()

            for q in range(4):
                part[n % 2, q] += prec[n, q].astype(F32)
            s1x[n % 2, 0] = part[n % 2, 2, top].astype(BF16)
            s1x[n % 2, 1] = part[n % 2, 3, top].astype(BF16)
            hop1_x(n).start()
            s1y[n % 2, 0] = part[n % 2, 1, low].astype(BF16)
            s1y[n % 2, 1] = part[n % 2, 3, low].astype(BF16)
            hop1_y(n).start()
            keep[n % 4, 0, top] = part[n % 2, 1, top]
            keep[n % 4, 0, low] = part[n % 2, 2, low]
            keep[n % 4, 1] = part[n % 2, 0]

        @pl.when((t >= 2) & (t < nn + 2))
        def _():
            n = t - 2

            @pl.when(n >= 2)
            def _():
                hop2_x(n - 2).wait_send()
                hop2_y(n - 2).wait_send()

            hop1_x(n).wait_recv()
            s2y[n % 2] = (keep[n % 4, 0, top] + r1x[n, 1].astype(F32)).astype(BF16)
            hop2_y(n).start()
            hop1_y(n).wait_recv()
            s2x[n % 2] = (keep[n % 4, 0, low] + r1y[n, 1].astype(F32)).astype(BF16)
            hop2_x(n).start()

        @pl.when((t >= 3) & (t < nn + 3))
        def _():
            n = t - 3
            at = pl.ds(pl.multiple_of(n * nc, nc), nc)
            hop2_y(n).wait_recv()
            o_ref[top, at] = (
                keep[n % 4, 1, top] + r1x[n, 0].astype(F32) + r2y[n].astype(F32)
            ).astype(BF16)
            hop2_x(n).wait_recv()
            o_ref[low, at] = (
                keep[n % 4, 1, low] + r1y[n, 0].astype(F32) + r2x[n].astype(F32)
            ).astype(BF16)

        @pl.when(t < nn)
        def _():
            n = t

            def two(q, _):
                got = []
                for b in range(2):
                    i = n * experts + 2 * q + b
                    d_copy(i).wait()
                    got.append(
                        jnp.dot(hid[2 * q + b], dring[i % DR], preferred_element_type=F32).reshape(8, slots, nc)
                    )
                outb[q] = jnp.concatenate(got, axis=1).astype(BF16)
                for b in range(2):
                    i = n * experts + 2 * q + b

                    @pl.when(i + DR < experts * nn)
                    def _():
                        d_copy(i + DR).start()

                return 0

            lax.fori_loop(0, experts // 2, two, 0)

            @pl.when(n >= 2)
            def _():
                to_part(n - 2).wait_send()

            for r in (1, 3, 5, 7, 0, 2, 4, 6):
                sums = jnp.dot(comb[r], outb[:, r].reshape(rows, nc), preferred_element_type=F32)
                if r % 2:
                    psend[n % 2, r // 2] = sums.astype(BF16)
                else:
                    part[n % 2, r // 2] = sums
                if r == 7:
                    to_part(n).start()

        return 0

    lax.fori_loop(0, nn + 3, reduce_step, 0)

    def drain(k, _):
        for copy in exchange:
            copy(k).wait_send()
        return 0

    lax.fori_loop(0, kn, drain, 0)
    for n in (nn - 2, nn - 1):
        for copy in (to_part, hop1_x, hop1_y, hop2_x, hop2_y):
            copy(n).wait_send()


def solution(mesh):
    def local(x, expert, slot, gate, w_gate, w_up, w_down):
        x = x.reshape(x.shape[-2:])
        tokens, d = x.shape
        top = expert.shape[-1]
        experts, _, ff = w_gate.shape
        total = experts * mesh.shape["ep"]
        slots = 5 * tokens * top // (4 * total)
        kc = nc = 256
        kn, nn = d // kc, d // nc
        rows, half = experts * slots, tokens // 2
        code = jnp.where(slot < slots, expert * slots + slot, -1).astype(F32)
        meta = jnp.concatenate([code, gate.astype(BF16).astype(F32)], axis=-1).reshape(tokens, 2 * top).T
        dma = pltpu.SemaphoreType.DMA
        any_ = pl.BlockSpec(memory_space=pl.ANY)
        y = pl.pallas_call(
            functools.partial(kernel, (tokens, d, ff, experts, slots, kc, nc)),
            out_shape=jax.ShapeDtypeStruct((tokens, d), BF16),
            in_specs=[any_] * 5,
            out_specs=pl.BlockSpec(memory_space=pltpu.VMEM),
            scratch_shapes=[
                pltpu.VMEM((8, 2 * top, tokens), F32),
                pltpu.VMEM((8, kn, tokens, kc), BF16),
                pltpu.VMEM((experts, 8 * slots, 2 * ff), F32),
                pltpu.VMEM((experts, 8 * slots, ff), BF16),
                pltpu.VMEM((experts, 8 * slots, kc), BF16),
                pltpu.VMEM((WR, 2, kc, ff), BF16),
                pltpu.VMEM((DR, ff, nc), BF16),
                pltpu.VMEM((8, rows, tokens), BF16),
                pltpu.VMEM((8, tokens, rows), BF16),
                pltpu.VMEM((experts // 2, 8, 2 * slots, nc), BF16),
                pltpu.VMEM((2, 4, tokens, nc), F32),
                pltpu.VMEM((2, 4, tokens, nc), BF16),
                pltpu.VMEM((nn, 4, tokens, nc), BF16),
                pltpu.VMEM((4, 2, tokens, nc), F32),
                pltpu.VMEM((2, 2, half, nc), BF16),
                pltpu.VMEM((2, 2, half, nc), BF16),
                pltpu.VMEM((nn, 2, half, nc), BF16),
                pltpu.VMEM((nn, 2, half, nc), BF16),
                pltpu.VMEM((2, half, nc), BF16),
                pltpu.VMEM((2, half, nc), BF16),
                pltpu.VMEM((nn, half, nc), BF16),
                pltpu.VMEM((nn, half, nc), BF16),
                dma((8,)), dma((8,)),
                dma((kn + 1,)),
                dma((8, kn)), dma((8, kn)),
                dma((WR, 2)), dma((DR,)),
                dma((nn,)), dma((nn,)),
                dma((2, nn)), dma((2, nn)), dma((2, nn)), dma((2, nn)),
            ],
            compiler_params=pltpu.CompilerParams(
                collective_id=0, has_side_effects=True, vmem_limit_bytes=67_000_000
            ),
        )(meta, x, w_gate, w_up, w_down)
        return y[None, None]

    tok = P("dp", "ep", None, None)
    ws = P("ep", None, None)
    return jax.shard_map(
        local, mesh=mesh, in_specs=(tok, tok, tok, tok, ws, ws, ws), out_specs=tok, check_vma=False
    )
```

```python
import functools

import jax
import jax.numpy as jnp
from jax import lax
from jax.experimental import pallas as pl
from jax.experimental.pallas import tpu as pltpu
from jax.sharding import PartitionSpec as P

MESH = pl.DeviceIdType.MESH
F32, BF16 = jnp.float32, jnp.bfloat16

CORE, Y, X = 1, 2, 4
WR, DR = 12, 8
L1, L2, L3 = 1, 3, 4
GROUP = 4


def kernel(
    cfg, expert_ref, slot_ref, gate_ref, x_ref, wg_ref, wu_ref, wd_ref, o_ref,
    meta, gates, xall, acc, hid, z, wring, dring, disp, comb, prec, r1x, r1y, r2x, r2y,
    meta_ss, meta_rs, load_s, ag_ss, ag_rs, wsem, dsem, p_ss, p_rs, h1_ss, h1_rs, h2_ss, h2_rs,
):
    tokens, d, ff, experts, slots, kc, nc = cfg
    rows = experts * slots
    kn, nn = d // kc, d // nc
    half = tokens // 2
    wide = 2 * slots
    dp, me = lax.axis_index("dp"), lax.axis_index("ep")

    def dev(mask):
        to = me
        for bit in (CORE, Y, X):
            if mask & bit:
                to = to + bit - 2 * bit * ((me // bit) % 2)
        return (dp, to)

    def remote(src, dst, ss, rs, mask):
        return pltpu.make_async_remote_copy(
            src_ref=src, dst_ref=dst, send_sem=ss, recv_sem=rs, device_id=dev(mask), device_id_type=MESH
        )

    def w_copies(i):
        e, k, slot = i % experts, i // experts, i % WR
        at = pl.ds(pl.multiple_of(k * kc, kc), kc)
        return (
            pltpu.make_async_copy(wg_ref.at[e, at], wring.at[slot, 0], wsem.at[slot, 0]),
            pltpu.make_async_copy(wu_ref.at[e, at], wring.at[slot, 1], wsem.at[slot, 1]),
        )

    def d_copy(i):
        e, n, slot = i % experts, i // experts, i % DR
        at = pl.ds(pl.multiple_of(n * nc, nc), nc)
        return pltpu.make_async_copy(wd_ref.at[e, :, at], dring.at[slot], dsem.at[slot])

    def to_x(k):
        return remote(xall.at[0, k], xall.at[X, k], ag_ss.at[0, k], ag_rs.at[0, k], X)

    def to_y(k):
        return remote(xall.at[0, k], xall.at[Y, k], ag_ss.at[1, k], ag_rs.at[1, k], Y)

    def to_core(k):
        return remote(xall.at[0, k], xall.at[CORE, k], ag_ss.at[2, k], ag_rs.at[2, k], CORE)

    def x_to_core(k):
        return remote(xall.at[X, k], xall.at[X | CORE, k], ag_ss.at[3, k], ag_rs.at[3, k], CORE)

    def y_to_core(k):
        return remote(xall.at[Y, k], xall.at[Y | CORE, k], ag_ss.at[4, k], ag_rs.at[4, k], CORE)

    def x_to_y(k):
        at = pl.ds(0, half)
        return remote(xall.at[X, k, at], xall.at[X | Y, k, at], ag_ss.at[5, k], ag_rs.at[5, k], Y)

    def y_to_x(k):
        at = pl.ds(half, half)
        return remote(xall.at[Y, k, at], xall.at[X | Y, k, at], ag_ss.at[6, k], ag_rs.at[6, k], X)

    def xy_to_core(k):
        return remote(xall.at[X | Y, k], xall.at[7, k], ag_ss.at[7, k], ag_rs.at[7, k], CORE)

    exchange = (to_x, to_y, to_core, x_to_core, y_to_core, x_to_y, y_to_x, xy_to_core)

    def own(k):
        at = pl.ds(pl.multiple_of(k * kc, kc), kc)
        return pltpu.make_async_copy(x_ref.at[:, at], xall.at[0, k], load_s.at[k])

    for k in range(kn):
        own(k).start()
    loads = [
        pltpu.make_async_copy(expert_ref, meta.at[0, 0], load_s.at[kn]),
        pltpu.make_async_copy(slot_ref, meta.at[0, 1], load_s.at[kn + 1]),
        pltpu.make_async_copy(gate_ref, gates.at[0], load_s.at[kn + 2]),
    ]
    for copy in loads:
        copy.start()
    for i in range(WR):
        for copy in w_copies(i):
            copy.start()

    barrier = pltpu.get_barrier_semaphore()
    for mask in range(1, 8):
        pl.semaphore_signal(barrier, inc=1, device_id=dev(mask), device_id_type=MESH)
    for copy in loads:
        copy.wait()
    pl.semaphore_wait(barrier, 7)

    metas = []
    for mask in range(1, 8):
        metas.append(remote(meta.at[0], meta.at[mask], meta_ss.at[0, mask], meta_rs.at[0, mask], mask))
        metas.append(remote(gates.at[0], gates.at[mask], meta_ss.at[1, mask], meta_rs.at[1, mask], mask))
    for copy in metas:
        copy.start()

    def first_hop(k):
        own(k).wait()
        to_x(k).start()
        to_y(k).start()
        to_core(k).start()

    first_hop(0)
    first_hop(1)

    def clear(e, _):
        acc[e] = jnp.zeros(acc.shape[1:], F32)
        return 0

    lax.fori_loop(0, experts, clear, 0)

    for copy in metas:
        copy.wait()

    def tables(r, _):
        row = lax.broadcasted_iota(jnp.int32, (rows, tokens), 0)
        slot = meta[r, 1]
        code = jnp.where(slot < slots, meta[r, 0] * slots + slot - me * rows, -1)
        gate = gates[r].astype(BF16).astype(F32)
        hit = jnp.zeros((rows, tokens), F32)
        weight = jnp.zeros((rows, tokens), F32)
        for j in range(8):
            same = code[j : j + 1] == row
            hit = jnp.where(same, 1.0, hit)
            weight = jnp.where(same, gate[j : j + 1], weight)
        disp[r] = hit.astype(BF16)
        comb[r] = jnp.transpose(weight).astype(BF16)
        return 0

    lax.fori_loop(0, 8, tables, 0)

    def place(k):
        for copy in (to_core, x_to_core, y_to_core, xy_to_core):
            copy(k).wait_recv()
        for pair in range(4):
            z0 = jnp.dot(disp[2 * pair], xall[2 * pair, k], preferred_element_type=F32)
            z1 = jnp.dot(disp[2 * pair + 1], xall[2 * pair + 1, k], preferred_element_type=F32)
            both = jnp.concatenate([z0.reshape(experts, slots, kc), z1.reshape(experts, slots, kc)], axis=1)
            z[:, pair * wide : (pair + 1) * wide, :] = both.astype(BF16)

    def project(k, run, last):
        first = k * experts + run * GROUP
        for b in range(GROUP):
            for copy in w_copies(first + b):
                copy.wait()
        step = 256
        for b in range(GROUP):
            e, ring = run * GROUP + b, (first + b) % WR
            lhs = z[e]
            for c in range(0, ff, step):
                at, up = slice(c, c + step), slice(ff + c, ff + c + step)
                g = acc[e, :, at] + jnp.dot(lhs, wring[ring, 0, :, at], preferred_element_type=F32)
                u = acc[e, :, up] + jnp.dot(lhs, wring[ring, 1, :, at], preferred_element_type=F32)
                if last:
                    hid[e, :, at] = (g * lax.logistic(g) * u).astype(BF16)
                else:
                    acc[e, :, at] = g
                    acc[e, :, up] = u
        if not last:
            for b in range(GROUP):

                @pl.when(first + b + WR < experts * kn)
                def _():
                    for copy in w_copies(first + b + WR):
                        copy.start()

    def gather_step(t, _):
        @pl.when(t < kn)
        def _():
            to_x(t).wait_recv()
            x_to_core(t).start()
            x_to_y(t).start()
            to_y(t).wait_recv()
            y_to_core(t).start()
            y_to_x(t).start()

        @pl.when(t + 2 < kn)
        def _():
            first_hop(t + 2)

        @pl.when(t >= 2)
        def _():
            project(t - 2, 1, False)

        @pl.when(t >= 1)
        def _():
            x_to_y(t - 1).wait_recv()
            y_to_x(t - 1).wait_recv()
            xy_to_core(t - 1).start()

        @pl.when((t >= 1) & (t < kn))
        def _():
            place(t - 1)
            project(t - 1, 0, False)

        return 0

    lax.fori_loop(0, kn + 1, gather_step, 0)
    for i in range(DR):
        d_copy(i).start()
    place(kn - 1)

    def last_step(run, _):
        project(kn - 1, run, True)
        return 0

    lax.fori_loop(0, experts // GROUP, last_step, 0)

    def drain(k, _):
        for copy in exchange:
            copy(k).wait_send()
        return 0

    lax.fori_loop(0, kn, drain, 0)

    top, low = pl.ds(0, half), pl.ds(half, half)

    def to_part(n, q):
        return remote(xall.at[2 * q + 1, n], prec.at[n, q], p_ss.at[n, q], p_rs.at[n, q], CORE)

    def hop1_x(n):
        return remote(xall.at[0, n], r1x.at[n], h1_ss.at[0, n], h1_rs.at[0, n], X)

    def hop1_y(n):
        return remote(xall.at[X, n], r1y.at[n], h1_ss.at[1, n], h1_rs.at[1, n], Y)

    def hop2_x(n):
        return remote(xall.at[Y, n, low], r2x.at[n], h2_ss.at[0, n], h2_rs.at[0, n], X)

    def hop2_y(n):
        return remote(xall.at[Y, n, top], r2y.at[n], h2_ss.at[1, n], h2_rs.at[1, n], Y)

    def col(q):
        return slice(q * nc, (q + 1) * nc)

    def last_projection(n):
        def run(g, _):
            first = n * experts + 4 * g
            for b in range(4):
                d_copy(first + b).wait()
            for a in range(2):
                got = [
                    jnp.dot(
                        hid[4 * g + 2 * a + b], dring[(first + 2 * a + b) % DR], preferred_element_type=F32
                    ).reshape(8, slots, nc)
                    for b in range(2)
                ]
                both = jnp.concatenate(got, axis=1).astype(BF16)
                for b in range(2):
                    z[4 * g + 2 * a + b] = both[4 * b : 4 * b + 4].reshape(8 * slots, nc)
            for b in range(4):

                @pl.when(first + b + DR < experts * nn)
                def _():
                    d_copy(first + b + DR).start()

            return 0

        lax.fori_loop(0, experts // 4, run, 0)
        for r in (1, 3, 5, 7, 0, 2, 4, 6):
            at = slice(r % 4 * wide, (r % 4 + 1) * wide)
            mine = jnp.concatenate([z[2 * q + r // 4, at] for q in range(experts // 2)], axis=0)
            sums = jnp.dot(comb[r], mine, preferred_element_type=F32)
            if r % 2:
                xall[r, n] = sums.astype(BF16)
                to_part(n, r // 2).start()
            else:
                acc[n, :tokens, col(r // 2)] = sums

    def sum_cores(n):
        for q in (3, 2, 1, 0):
            to_part(n, q).wait_recv()
            both = acc[n, :tokens, col(q)] + prec[n, q].astype(F32)
            acc[n, :tokens, col(q)] = both
            both = both.astype(BF16)
            if q == 3:
                xall[0, n, low] = both[:half]
                xall[X, n, low] = both[half:]
            if q == 2:
                xall[0, n, top] = both[:half]
                hop1_x(n).start()
            if q == 1:
                xall[X, n, top] = both[half:]
                hop1_y(n).start()

    def sum_first(n):
        hop1_x(n).wait_recv()
        xall[Y, n, top] = (acc[n, top, col(1)] + r1x[n, low].astype(F32)).astype(BF16)
        hop2_y(n).start()
        hop1_y(n).wait_recv()
        xall[Y, n, low] = (acc[n, low, col(2)] + r1y[n, low].astype(F32)).astype(BF16)
        hop2_x(n).start()

    def sum_second(n):
        at = pl.ds(pl.multiple_of(n * nc, nc), nc)
        hop2_y(n).wait_recv()
        o_ref[top, at] = (acc[n, top, col(0)] + r1x[n, top].astype(F32) + r2y[n].astype(F32)).astype(BF16)
        hop2_x(n).wait_recv()
        o_ref[low, at] = (acc[n, low, col(0)] + r1y[n, top].astype(F32) + r2x[n].astype(F32)).astype(BF16)

    def reduce_step(t, _):
        for lag, stage in ((L1, sum_cores), (L2, sum_first), (L3, sum_second), (0, last_projection)):

            @pl.when((t >= lag) & (t < nn + lag))
            def _():
                stage(t - lag)

        return 0

    lax.fori_loop(0, nn + L3, reduce_step, 0)

    def drain_sums(n, _):
        for q in range(4):
            to_part(n, q).wait_send()
        for copy in (hop1_x, hop1_y, hop2_x, hop2_y):
            copy(n).wait_send()
        return 0

    lax.fori_loop(0, nn, drain_sums, 0)


def solution(mesh):
    def local(x, expert, slot, gate, w_gate, w_up, w_down):
        x = x.reshape(x.shape[-2:])
        tokens, d = x.shape
        top = expert.shape[-1]
        experts, _, ff = w_gate.shape
        total = experts * mesh.shape["ep"]
        slots = 5 * tokens * top // (4 * total)
        kc = nc = 256
        kn, nn = d // kc, d // nc
        rows, half = experts * slots, tokens // 2
        expert, slot, gate = (v.reshape(tokens, top).T for v in (expert, slot, gate))
        dma = pltpu.SemaphoreType.DMA
        any_ = pl.BlockSpec(memory_space=pl.ANY)
        y = pl.pallas_call(
            functools.partial(kernel, (tokens, d, ff, experts, slots, kc, nc)),
            out_shape=jax.ShapeDtypeStruct((tokens, d), BF16),
            in_specs=[any_] * 7,
            out_specs=pl.BlockSpec(memory_space=pltpu.VMEM),
            scratch_shapes=[
                pltpu.VMEM((8, 2, top, tokens), jnp.int32),
                pltpu.VMEM((8, top, tokens), F32),
                pltpu.VMEM((8, kn, tokens, kc), BF16),
                pltpu.VMEM((experts, 8 * slots, 2 * ff), F32),
                pltpu.VMEM((experts, 8 * slots, ff), BF16),
                pltpu.VMEM((experts, 8 * slots, kc), BF16),
                pltpu.VMEM((WR, 2, kc, ff), BF16),
                pltpu.VMEM((DR, ff, nc), BF16),
                pltpu.VMEM((8, rows, tokens), BF16),
                pltpu.VMEM((8, tokens, rows), BF16),
                pltpu.VMEM((nn, 4, tokens, nc), BF16),
                pltpu.VMEM((nn, tokens, nc), BF16),
                pltpu.VMEM((nn, tokens, nc), BF16),
                pltpu.VMEM((nn, half, nc), BF16),
                pltpu.VMEM((nn, half, nc), BF16),
                dma((2, 8)), dma((2, 8)),
                dma((kn + 3,)),
                dma((8, kn)), dma((8, kn)),
                dma((WR, 2)), dma((DR,)),
                dma((nn, 4)), dma((nn, 4)),
                dma((2, nn)), dma((2, nn)), dma((2, nn)), dma((2, nn)),
            ],
            compiler_params=pltpu.CompilerParams(
                collective_id=0, has_side_effects=True, vmem_limit_bytes=67_000_000
            ),
        )(expert, slot, gate, x, w_gate, w_up, w_down)
        return y[None, None]

    tok = P("dp", "ep", None, None)
    ws = P("ep", None, None)
    return jax.shard_map(
        local, mesh=mesh, in_specs=(tok, tok, tok, tok, ws, ws, ws), out_specs=tok, check_vma=False
    )
```

```python
import functools

import jax
import jax.numpy as jnp
from jax import lax
from jax.experimental import pallas as pl
from jax.experimental.pallas import tpu as pltpu
from jax.sharding import PartitionSpec as P

MESH = pl.DeviceIdType.MESH
F32, BF16 = jnp.float32, jnp.bfloat16

CORE, Y, X = 1, 2, 4
WR, DR = 12, 8
L2, L3 = 2, 5
GROUP = 4


def kernel(
    cfg, expert_ref, slot_ref, gate_ref, x_ref, wg_ref, wu_ref, wd_ref, o_ref,
    raw, rawg, codes, gates, xall, acc, hid, z, wring, dring, disp, comb, prec, r1, r2,
    meta_ss, meta_rs, load_s, send_s, ag_rs, wsem, dsem, p_rs, h1_rs, h2_rs, out_s,
):
    tokens, d, ff, experts, slots, kc, nc = cfg
    rows = experts * slots
    kn, nn = d // kc, d // nc
    half = tokens // 2
    wide = 2 * slots
    dp, me = lax.axis_index("dp"), lax.axis_index("ep")

    def dev(mask):
        to = me
        for bit in (CORE, Y, X):
            if mask & bit:
                to = to + bit - 2 * bit * ((me // bit) % 2)
        return (dp, to)

    def remote(src, dst, ss, rs, mask):
        return pltpu.make_async_remote_copy(
            src_ref=src, dst_ref=dst, send_sem=ss, recv_sem=rs, device_id=dev(mask), device_id_type=MESH
        )

    def landed(ref, sem):
        pltpu.make_async_copy(ref, ref, sem).wait()

    def w_start(first):
        for b in range(GROUP):
            i = first + b
            e, k, ring = i % experts, i // experts, i % WR
            at = pl.ds(pl.multiple_of(k * kc, kc), kc)
            sem = wsem.at[first // GROUP % (WR // GROUP)]
            pltpu.make_async_copy(wg_ref.at[e, at], wring.at[ring, 0], sem).start()
            pltpu.make_async_copy(wu_ref.at[e, at], wring.at[ring, 1], sem).start()

    def w_wait(first):
        landed(wring.at[pl.ds(first % WR, GROUP)], wsem.at[first // GROUP % (WR // GROUP)])

    def d_start(first):
        for b in range(4):
            i = first + b
            e, n, ring = i % experts, i // experts, i % DR
            at = pl.ds(pl.multiple_of(n * nc, nc), nc)
            pltpu.make_async_copy(wd_ref.at[e, :, at], dring.at[ring], dsem.at[first // 4 % (DR // 4)]).start()

    def d_wait(first):
        landed(dring.at[pl.ds(first % DR, 4)], dsem.at[first // 4 % (DR // 4)])

    top, low = pl.ds(0, half), pl.ds(half, half)

    def exchange(kind, src, dst, k, mask, at=None):
        src, dst = xall.at[src, k], xall.at[dst, k]
        if at is not None:
            src, dst = src.at[at], dst.at[at]
        return remote(src, dst, send_s, ag_rs.at[kind, k], mask)

    def first_x(k):
        return exchange(0, 0, X, k, X, top)

    def first_y(k):
        return exchange(0, 0, Y, k, Y, low)

    def second_x(k):
        return exchange(1, 0, X, k, X, low)

    def second_y(k):
        return exchange(1, 0, Y, k, Y, top)

    def to_core(k):
        return exchange(2, 0, CORE, k, CORE)

    def x_to_core(k):
        return exchange(2, X, X | CORE, k, CORE)

    def y_to_core(k):
        return exchange(2, Y, Y | CORE, k, CORE)

    def x_to_y(k):
        return exchange(3, X, X | Y, k, Y, top)

    def y_to_x(k):
        return exchange(3, Y, X | Y, k, X, low)

    def xy_to_core(k):
        return exchange(2, X | Y, 7, k, CORE)

    def own_start(k):
        at = pl.ds(pl.multiple_of(k * kc, kc), kc)
        pltpu.make_async_copy(x_ref.at[:, at], xall.at[0, k], load_s.at[3 + min(k, 2)]).start()

    loads = [
        pltpu.make_async_copy(expert_ref, raw.at[0], load_s.at[0]),
        pltpu.make_async_copy(slot_ref, raw.at[1], load_s.at[1]),
        pltpu.make_async_copy(gate_ref, rawg, load_s.at[2]),
    ]
    for copy in loads:
        copy.start()
    for k in range(2):
        own_start(k)
    barrier = pltpu.get_barrier_semaphore()
    for mask in range(1, 8):
        pl.semaphore_signal(barrier, inc=1, device_id=dev(mask), device_id_type=MESH)
    for copy in loads:
        copy.wait()
    codes[0] = jnp.where(raw[1] < slots, raw[0] * slots + raw[1], -1)
    gates[0] = rawg[...].astype(BF16)
    pl.semaphore_wait(barrier, 7)

    def send_codes(mask):
        return remote(codes.at[0], codes.at[mask], meta_ss.at[0], meta_rs.at[0], mask)

    def send_gates(mask):
        return remote(gates.at[0], gates.at[mask], meta_ss.at[1], meta_rs.at[1], mask)

    def send_first(k):
        first_x(k).start()
        first_y(k).start()

    def send_second(k):
        second_x(k).start()
        second_y(k).start()
        to_core(k).start()

    for mask in (6, 7, 4, 5, 2, 3, 1):
        send_codes(mask).start()
    landed(xall.at[0, 0], load_s.at[3])
    send_first(0)
    for mask in (6, 7, 4, 5, 2, 3, 1):
        send_gates(mask).start()
    send_second(0)
    landed(xall.at[0, 1], load_s.at[4])
    send_first(1)
    for k in range(2, kn):
        own_start(k)
    for i in range(0, WR, GROUP):
        w_start(i)

    def clear(e, _):
        acc[e] = jnp.zeros(acc.shape[1:], F32)
        return 0

    lax.fori_loop(0, experts, clear, 0)

    def table(r, values):
        row = lax.broadcasted_iota(jnp.int32, (rows, tokens), 0)
        code = codes[r] - me * rows
        out = jnp.zeros((rows, tokens), F32)
        for j in range(8):
            out = jnp.where(code[j : j + 1] == row, 1.0 if values is None else values[j : j + 1], out)
        return out

    def dispatch_table(r, _):
        disp[r] = table(r, None).astype(BF16)
        return 0

    def combine_table(r, _):
        comb[r] = jnp.transpose(table(r, gates[r].astype(F32))).astype(BF16)
        return 0

    landed(codes.at[pl.ds(1, 7)], meta_rs.at[0])
    lax.fori_loop(0, 8, dispatch_table, 0)

    def place(k):
        landed(xall.at[pl.ds(0, 4), k], ag_rs.at[2, k])
        for pair in range(4):
            z0 = jnp.dot(disp[2 * pair], xall[2 * pair, k], preferred_element_type=F32)
            z1 = jnp.dot(disp[2 * pair + 1], xall[2 * pair + 1, k], preferred_element_type=F32)
            both = jnp.concatenate([z0.reshape(experts, slots, kc), z1.reshape(experts, slots, kc)], axis=1)
            z[:, pair * wide : (pair + 1) * wide, :] = both.astype(BF16)

    def project(k, run, last):
        first = k * experts + run * GROUP
        w_wait(first)
        step = 256 if last else 512
        for b in range(GROUP):
            e, ring = run * GROUP + b, (first + b) % WR
            lhs = z[e]
            for c in range(0, ff, step):
                at, up = slice(c, c + step), slice(ff + c, ff + c + step)
                g = acc[e, :, at] + jnp.dot(lhs, wring[ring, 0, :, at], preferred_element_type=F32)
                u = acc[e, :, up] + jnp.dot(lhs, wring[ring, 1, :, at], preferred_element_type=F32)
                if last:
                    hid[e, :, at] = (g * lax.logistic(g) * u).astype(BF16)
                else:
                    acc[e, :, at] = g
                    acc[e, :, up] = u
        if not last:

            @pl.when(first + WR < experts * kn)
            def _():
                w_start(first + WR)

    def pass_first(k):
        landed(xall.at[0, k], ag_rs.at[0, k])
        x_to_y(k).start()
        y_to_x(k).start()

        @pl.when(k + 1 < kn)
        def _():
            send_second(k + 1)

    def pass_second(k):
        landed(xall.at[0, k], ag_rs.at[1, k])
        x_to_core(k).start()
        y_to_core(k).start()

        @pl.when(k + 2 < kn)
        def _():
            send_first(k + 2)

    def pass_across(k):
        landed(xall.at[X | Y, k], ag_rs.at[3, k])
        xy_to_core(k).start()

    def gather_step(t, _):
        @pl.when(t < kn)
        def _():
            pass_first(t)

        @pl.when(t >= 2)
        def _():
            project(t - 2, 0, False)

        pass_across(t - 1)

        @pl.when(t >= 2)
        def _():
            project(t - 2, 1, False)

        @pl.when(t < kn)
        def _():
            pass_second(t)

        place(t - 1)
        return 0

    pass_first(0)
    landed(xall.at[0, pl.ds(2, kn - 2)], load_s.at[5])
    pass_second(0)
    landed(gates.at[pl.ds(1, 7)], meta_rs.at[1])
    lax.fori_loop(0, 8, combine_table, 0)
    lax.fori_loop(1, kn + 1, gather_step, 0)
    for i in range(0, DR, 4):
        d_start(i)

    def last_step(run, _):
        project(kn - 1, run, True)
        return 0

    lax.fori_loop(0, experts // GROUP, last_step, 0)

    landed(xall.at[pl.ds(0, 7)], send_s)
    landed(codes.at[pl.ds(1, 7)], meta_ss.at[0])
    landed(gates.at[pl.ds(1, 7)], meta_ss.at[1])

    def to_part(n, q):
        return remote(xall.at[2 * q + 1, n], prec.at[n, q], send_s, p_rs.at[n], CORE)

    def hop1_x(n):
        return remote(xall.at[0, n], r1.at[n, 0], send_s, h1_rs.at[n], X)

    def hop1_y(n):
        return remote(xall.at[X, n], r1.at[n, 1], send_s, h1_rs.at[n], Y)

    def hop2_x(n):
        return remote(xall.at[Y, n, low], r2.at[n, 0], send_s, h2_rs.at[n], X)

    def hop2_y(n):
        return remote(xall.at[Y, n, top], r2.at[n, 1], send_s, h2_rs.at[n], Y)

    def col(q):
        return slice(q * nc, (q + 1) * nc)

    def last_projection(g, n):
        first = n * experts + 4 * g
        d_wait(first)
        for a in range(2):
            got = [
                jnp.dot(
                    hid[4 * g + 2 * a + b], dring[(first + 2 * a + b) % DR], preferred_element_type=F32
                ).reshape(8, slots, nc)
                for b in range(2)
            ]
            both = jnp.concatenate(got, axis=1).astype(BF16)
            for b in range(2):
                z[4 * g + 2 * a + b] = both[4 * b : 4 * b + 4].reshape(8 * slots, nc)

        @pl.when(first + DR < experts * nn)
        def _():
            d_start(first + DR)

    def combine(n):
        def sums(r):
            at = slice(r % 4 * wide, (r % 4 + 1) * wide)
            mine = jnp.concatenate([z[2 * q + r // 4, at] for q in range(experts // 2)], axis=0)
            return jnp.dot(comb[r], mine, preferred_element_type=F32)

        for r in (7, 5, 3, 1):
            xall[r, n] = sums(r).astype(BF16)
        for r in (7, 5, 3, 1):
            to_part(n, r // 2).start()
        for r in (6, 4, 2, 0):
            acc[n, :tokens, col(r // 2)] = sums(r)

    def sum_cores(n):
        landed(prec.at[n], p_rs.at[n])
        for q in (3, 2, 1, 0):
            both = acc[n, :tokens, col(q)] + prec[n, q].astype(F32)
            acc[n, :tokens, col(q)] = both
            both = both.astype(BF16)
            if q == 3:
                xall[0, n, low] = both[:half]
                xall[X, n, low] = both[half:]
            if q == 2:
                xall[0, n, top] = both[:half]
                hop1_x(n).start()
            if q == 1:
                xall[X, n, top] = both[half:]
                hop1_y(n).start()

    def sum_first(n):
        landed(r1.at[n], h1_rs.at[n])
        xall[Y, n, top] = (acc[n, top, col(1)] + r1[n, 0, low].astype(F32)).astype(BF16)
        hop2_y(n).start()
        xall[Y, n, low] = (acc[n, low, col(2)] + r1[n, 1, low].astype(F32)).astype(BF16)
        hop2_x(n).start()

    def put(n):
        at = pl.ds(pl.multiple_of(n * nc, nc), nc)
        return pltpu.make_async_copy(prec.at[n, 0], o_ref.at[:, at], out_s)

    def sum_second(n):
        landed(r2.at[n], h2_rs.at[n])
        prec[n, 0, top] = (acc[n, top, col(0)] + r1[n, 0, top].astype(F32) + r2[n, 1].astype(F32)).astype(BF16)
        prec[n, 0, low] = (acc[n, low, col(0)] + r1[n, 1, top].astype(F32) + r2[n, 0].astype(F32)).astype(BF16)
        put(n).start()

    stages = (
        (0, functools.partial(last_projection, 0)), (1, sum_cores), (0, functools.partial(last_projection, 1)),
        (0, combine), (L2, sum_first), (L3, sum_second),
    )

    def reduce_step(t, _):
        for lag, stage in stages:

            @pl.when((t >= lag) & (t < nn + lag))
            def _():
                stage(t - lag)

        return 0

    lax.fori_loop(0, nn + L3, reduce_step, 0)

    landed(xall.at[pl.ds(0, 7)], send_s)
    landed(xall.at[0], out_s)


def solution(mesh):
    def local(x, expert, slot, gate, w_gate, w_up, w_down):
        x = x.reshape(x.shape[-2:])
        tokens, d = x.shape
        top = expert.shape[-1]
        experts, _, ff = w_gate.shape
        total = experts * mesh.shape["ep"]
        slots = 5 * tokens * top // (4 * total)
        kc = nc = 256
        kn, nn = d // kc, d // nc
        rows, half = experts * slots, tokens // 2
        expert, slot, gate = (v.reshape(tokens, top).T for v in (expert, slot, gate))
        dma = pltpu.SemaphoreType.DMA
        any_ = pl.BlockSpec(memory_space=pl.ANY)
        y = pl.pallas_call(
            functools.partial(kernel, (tokens, d, ff, experts, slots, kc, nc)),
            out_shape=jax.ShapeDtypeStruct((tokens, d), BF16),
            in_specs=[any_] * 7,
            out_specs=any_,
            scratch_shapes=[
                pltpu.VMEM((2, top, tokens), jnp.int32),
                pltpu.VMEM((top, tokens), F32),
                pltpu.VMEM((8, top, tokens), jnp.int32),
                pltpu.VMEM((8, top, tokens), BF16),
                pltpu.VMEM((8, kn, tokens, kc), BF16),
                pltpu.VMEM((experts, 8 * slots, 2 * ff), F32),
                pltpu.VMEM((experts, 8 * slots, ff), BF16),
                pltpu.VMEM((experts, 8 * slots, kc), BF16),
                pltpu.VMEM((WR, 2, kc, ff), BF16),
                pltpu.VMEM((DR, ff, nc), BF16),
                pltpu.VMEM((8, rows, tokens), BF16),
                pltpu.VMEM((8, tokens, rows), BF16),
                pltpu.VMEM((nn, 4, tokens, nc), BF16),
                pltpu.VMEM((nn, 2, tokens, nc), BF16),
                pltpu.VMEM((nn, 2, half, nc), BF16),
                dma((2,)), dma((2,)),
                dma((6,)),
                dma,
                dma((4, kn)),
                dma((WR // GROUP,)), dma((DR // 4,)),
                dma((nn,)), dma((nn,)), dma((nn,)),
                dma,
            ],
            compiler_params=pltpu.CompilerParams(
                collective_id=0, has_side_effects=True, vmem_limit_bytes=67_000_000
            ),
        )(expert, slot, gate, x, w_gate, w_up, w_down)
        return y[None, None]

    tok = P("dp", "ep", None, None)
    ws = P("ep", None, None)
    return jax.shard_map(
        local, mesh=mesh, in_specs=(tok, tok, tok, tok, ws, ws, ws), out_specs=tok, check_vma=False
    )
```

```python
import functools

import jax
import jax.numpy as jnp
from jax import lax
from jax.experimental import pallas as pl
from jax.experimental.pallas import tpu as pltpu
from jax.sharding import PartitionSpec as P

MESH = pl.DeviceIdType.MESH
F32, BF16 = jnp.float32, jnp.bfloat16

CORE, Y, X = 1, 2, 4
WR, DR = 12, 8
L2, L3 = 2, 5
GROUP = 4


def kernel(
    cfg, expert_ref, slot_ref, gate_ref, x_ref, wg_ref, wu_ref, wd_ref, o_ref,
    raw, rawg, codes, gates, xall, acc, hid, z, wring, dring, disp, comb, prec, r1, r2,
    meta_ss, meta_rs, load_s, send_s, ag_rs, wsem, dsem, p_rs, h1_rs, h2_rs,
):
    tokens, d, ff, experts, slots, kc, nc = cfg
    rows = experts * slots
    kn, nn = d // kc, d // nc
    half = tokens // 2
    wide = 2 * slots
    dp, me = lax.axis_index("dp"), lax.axis_index("ep")

    def dev(mask):
        to = me
        for bit in (CORE, Y, X):
            if mask & bit:
                to = to + bit - 2 * bit * ((me // bit) % 2)
        return (dp, to)

    def remote(src, dst, ss, rs, mask):
        return pltpu.make_async_remote_copy(
            src_ref=src, dst_ref=dst, send_sem=ss, recv_sem=rs, device_id=dev(mask), device_id_type=MESH
        )

    def landed(ref, sem):
        pltpu.make_async_copy(ref, ref, sem).wait()

    def w_start(first):
        for b in range(GROUP):
            i = first + b
            e, k, ring = i % experts, i // experts, i % WR
            at = pl.ds(pl.multiple_of(k * kc, kc), kc)
            sem = wsem.at[first // GROUP % (WR // GROUP)]
            pltpu.make_async_copy(wg_ref.at[e, at], wring.at[ring, 0], sem).start()
            pltpu.make_async_copy(wu_ref.at[e, at], wring.at[ring, 1], sem).start()

    def w_wait(first):
        landed(wring.at[pl.ds(first % WR, GROUP)], wsem.at[first // GROUP % (WR // GROUP)])

    def d_start(first):
        for b in range(4):
            i = first + b
            e, n, ring = i % experts, i // experts, i % DR
            at = pl.ds(pl.multiple_of(n * nc, nc), nc)
            pltpu.make_async_copy(wd_ref.at[e, :, at], dring.at[ring], dsem.at[first // 4 % (DR // 4)]).start()

    def d_wait(first):
        landed(dring.at[pl.ds(first % DR, 4)], dsem.at[first // 4 % (DR // 4)])

    top, low = pl.ds(0, half), pl.ds(half, half)

    def exchange(kind, src, dst, k, mask, at=None):
        src, dst = xall.at[src, k], xall.at[dst, k]
        if at is not None:
            src, dst = src.at[at], dst.at[at]
        return remote(src, dst, send_s, ag_rs.at[kind, k], mask)

    def first_x(k):
        return exchange(0, 0, X, k, X, top)

    def first_y(k):
        return exchange(0, 0, Y, k, Y, low)

    def second_x(k):
        return exchange(1, 0, X, k, X, low)

    def second_y(k):
        return exchange(1, 0, Y, k, Y, top)

    def to_core(k):
        return exchange(2, 0, CORE, k, CORE)

    def x_to_core(k):
        return exchange(2, X, X | CORE, k, CORE)

    def y_to_core(k):
        return exchange(2, Y, Y | CORE, k, CORE)

    def x_to_y(k):
        return exchange(3, X, X | Y, k, Y, top)

    def y_to_x(k):
        return exchange(3, Y, X | Y, k, X, low)

    def xy_to_core(k):
        return exchange(2, X | Y, 7, k, CORE)

    def own_start(k):
        at = pl.ds(pl.multiple_of(k * kc, kc), kc)
        pltpu.make_async_copy(x_ref.at[:, at], xall.at[0, k], load_s.at[3 + min(k, 2)]).start()

    loads = [
        pltpu.make_async_copy(expert_ref, raw.at[0], load_s.at[0]),
        pltpu.make_async_copy(slot_ref, raw.at[1], load_s.at[1]),
        pltpu.make_async_copy(gate_ref, rawg, load_s.at[2]),
    ]
    for copy in loads:
        copy.start()
    for k in range(2):
        own_start(k)
    barrier = pltpu.get_barrier_semaphore()
    for mask in range(1, 8):
        pl.semaphore_signal(barrier, inc=1, device_id=dev(mask), device_id_type=MESH)
    for copy in loads:
        copy.wait()
    codes[0] = jnp.where(raw[1] < slots, raw[0] * slots + raw[1], -1)
    gates[0] = rawg[...].astype(BF16)
    pl.semaphore_wait(barrier, 7)

    def send_codes(mask):
        return remote(codes.at[0], codes.at[mask], meta_ss.at[0], meta_rs.at[0], mask)

    def send_gates(mask):
        return remote(gates.at[0], gates.at[mask], meta_ss.at[1], meta_rs.at[1], mask)

    def send_first(k):
        first_x(k).start()
        first_y(k).start()

    def send_second(k):
        second_x(k).start()
        second_y(k).start()
        to_core(k).start()

    for mask in (6, 7, 4, 5, 2, 3, 1):
        send_codes(mask).start()
    landed(xall.at[0, 0], load_s.at[3])
    send_first(0)
    for mask in (6, 7, 4, 5, 2, 3, 1):
        send_gates(mask).start()
    send_second(0)
    landed(xall.at[0, 1], load_s.at[4])
    send_first(1)
    for k in range(2, kn):
        own_start(k)
    for i in range(0, WR, GROUP):
        w_start(i)

    def clear(e, _):
        acc[e] = jnp.zeros(acc.shape[1:], F32)
        return 0

    lax.fori_loop(0, experts, clear, 0)

    def table(r, values):
        row = lax.broadcasted_iota(jnp.int32, (rows, tokens), 0)
        code = codes[r] - me * rows
        out = jnp.zeros((rows, tokens), F32)
        for j in range(8):
            out = jnp.where(code[j : j + 1] == row, 1.0 if values is None else values[j : j + 1], out)
        return out

    def dispatch_table(r, _):
        disp[r] = table(r, None).astype(BF16)
        return 0

    def combine_table(r, _):
        comb[r] = jnp.transpose(table(r, gates[r].astype(F32))).astype(BF16)
        return 0

    landed(codes.at[pl.ds(1, 7)], meta_rs.at[0])
    lax.fori_loop(0, 8, dispatch_table, 0)

    def place(k):
        landed(xall.at[pl.ds(0, 4), k], ag_rs.at[2, k])
        for pair in range(4):
            z0 = jnp.dot(disp[2 * pair], xall[2 * pair, k], preferred_element_type=F32)
            z1 = jnp.dot(disp[2 * pair + 1], xall[2 * pair + 1, k], preferred_element_type=F32)
            both = jnp.concatenate([z0.reshape(experts, slots, kc), z1.reshape(experts, slots, kc)], axis=1)
            z[:, pair * wide : (pair + 1) * wide, :] = both.astype(BF16)

    def project(k, run, last):
        first = k * experts + run * GROUP
        w_wait(first)
        step = 256 if last else 512
        for b in range(GROUP):
            e, ring = run * GROUP + b, (first + b) % WR
            lhs = z[e]
            for c in range(0, ff, step):
                at, up = slice(c, c + step), slice(ff + c, ff + c + step)
                g = acc[e, :, at] + jnp.dot(lhs, wring[ring, 0, :, at], preferred_element_type=F32)
                u = acc[e, :, up] + jnp.dot(lhs, wring[ring, 1, :, at], preferred_element_type=F32)
                if last:
                    hid[e, :, at] = (g * lax.logistic(g) * u).astype(BF16)
                else:
                    acc[e, :, at] = g
                    acc[e, :, up] = u
        if not last:

            @pl.when(first + WR < experts * kn)
            def _():
                w_start(first + WR)

    def pass_first(k):
        landed(xall.at[0, k], ag_rs.at[0, k])
        x_to_y(k).start()
        y_to_x(k).start()

        @pl.when(k + 1 < kn)
        def _():
            send_second(k + 1)

    def pass_second(k):
        landed(xall.at[0, k], ag_rs.at[1, k])
        x_to_core(k).start()
        y_to_core(k).start()

        @pl.when(k + 2 < kn)
        def _():
            send_first(k + 2)

    def pass_across(k):
        landed(xall.at[X | Y, k], ag_rs.at[3, k])
        xy_to_core(k).start()

    def gather_step(t, _):
        @pl.when(t >= 2)
        def _():
            project(t - 2, 0, False)

        @pl.when(t < kn)
        def _():
            pass_first(t)

        pass_across(t - 1)

        @pl.when(t >= 2)
        def _():
            project(t - 2, 1, False)

        @pl.when(t < kn)
        def _():
            pass_second(t)

        place(t - 1)
        return 0

    pass_first(0)
    landed(xall.at[0, pl.ds(2, kn - 2)], load_s.at[5])
    pass_second(0)
    landed(gates.at[pl.ds(1, 7)], meta_rs.at[1])
    lax.fori_loop(0, 8, combine_table, 0)
    lax.fori_loop(1, kn + 1, gather_step, 0)
    for i in range(0, DR, 4):
        d_start(i)

    def last_step(run, _):
        project(kn - 1, run, True)
        return 0

    lax.fori_loop(0, experts // GROUP, last_step, 0)

    landed(xall.at[pl.ds(0, 7)], send_s)
    landed(codes.at[pl.ds(1, 7)], meta_ss.at[0])
    landed(gates.at[pl.ds(1, 7)], meta_ss.at[1])

    def to_part(n, q):
        return remote(xall.at[2 * q + 1, n], prec.at[n, q], send_s, p_rs.at[n], CORE)

    def hop1_x(n):
        return remote(xall.at[0, n], r1.at[n, 0], send_s, h1_rs.at[n], X)

    def hop1_y(n):
        return remote(xall.at[X, n], r1.at[n, 1], send_s, h1_rs.at[n], Y)

    def hop2_x(n):
        return remote(xall.at[Y, n, low], r2.at[n, 0], send_s, h2_rs.at[n], X)

    def hop2_y(n):
        return remote(xall.at[Y, n, top], r2.at[n, 1], send_s, h2_rs.at[n], Y)

    def col(q):
        return slice(q * nc, (q + 1) * nc)

    def last_projection(g, n):
        first = n * experts + 4 * g
        d_wait(first)
        for a in range(2):
            got = [
                jnp.dot(
                    hid[4 * g + 2 * a + b], dring[(first + 2 * a + b) % DR], preferred_element_type=F32
                ).reshape(8, slots, nc)
                for b in range(2)
            ]
            both = jnp.concatenate(got, axis=1).astype(BF16)
            for b in range(2):
                z[4 * g + 2 * a + b] = both[4 * b : 4 * b + 4].reshape(8 * slots, nc)

        @pl.when(first + DR < experts * nn)
        def _():
            d_start(first + DR)

    def combine(n):
        def sums(r):
            at = slice(r % 4 * wide, (r % 4 + 1) * wide)
            mine = jnp.concatenate([z[2 * q + r // 4, at] for q in range(experts // 2)], axis=0)
            return jnp.dot(comb[r], mine, preferred_element_type=F32)

        for r in (7, 5, 3, 1):
            xall[r, n] = sums(r).astype(BF16)
        for r in (7, 5, 3, 1):
            to_part(n, r // 2).start()
        for r in (6, 4, 2, 0):
            acc[n, :tokens, col(r // 2)] = sums(r)

    def sum_cores(n):
        landed(prec.at[n], p_rs.at[n])
        for q in (3, 2, 1, 0):
            both = acc[n, :tokens, col(q)] + prec[n, q].astype(F32)
            acc[n, :tokens, col(q)] = both
            both = both.astype(BF16)
            if q == 3:
                xall[0, n, low] = both[:half]
                xall[X, n, low] = both[half:]
            if q == 2:
                xall[0, n, top] = both[:half]
                hop1_x(n).start()
            if q == 1:
                xall[X, n, top] = both[half:]
                hop1_y(n).start()

    def sum_first(n):
        landed(r1.at[n], h1_rs.at[n])
        xall[Y, n, top] = (acc[n, top, col(1)] + r1[n, 0, low].astype(F32)).astype(BF16)
        hop2_y(n).start()
        xall[Y, n, low] = (acc[n, low, col(2)] + r1[n, 1, low].astype(F32)).astype(BF16)
        hop2_x(n).start()

    def sum_second(n):
        at = pl.ds(pl.multiple_of(n * nc, nc), nc)
        landed(r2.at[n], h2_rs.at[n])
        o_ref[top, at] = (acc[n, top, col(0)] + r1[n, 0, top].astype(F32) + r2[n, 1].astype(F32)).astype(BF16)
        o_ref[low, at] = (acc[n, low, col(0)] + r1[n, 1, top].astype(F32) + r2[n, 0].astype(F32)).astype(BF16)

    stages = (
        (0, functools.partial(last_projection, 0)), (1, sum_cores), (0, functools.partial(last_projection, 1)),
        (0, combine), (L2, sum_first), (L3, sum_second),
    )

    def reduce_step(t, _):
        for lag, stage in stages:

            @pl.when((t >= lag) & (t < nn + lag))
            def _():
                stage(t - lag)

        return 0

    lax.fori_loop(0, nn + L3, reduce_step, 0)

    landed(xall.at[pl.ds(0, 7)], send_s)


def solution(mesh):
    def local(x, expert, slot, gate, w_gate, w_up, w_down):
        x = x.reshape(x.shape[-2:])
        tokens, d = x.shape
        top = expert.shape[-1]
        experts, _, ff = w_gate.shape
        total = experts * mesh.shape["ep"]
        slots = 5 * tokens * top // (4 * total)
        kc = nc = 256
        kn, nn = d // kc, d // nc
        rows, half = experts * slots, tokens // 2
        expert, slot, gate = (v.reshape(tokens, top).T for v in (expert, slot, gate))
        dma = pltpu.SemaphoreType.DMA
        any_ = pl.BlockSpec(memory_space=pl.ANY)
        y = pl.pallas_call(
            functools.partial(kernel, (tokens, d, ff, experts, slots, kc, nc)),
            out_shape=pltpu.VMEM((tokens, d), BF16),
            in_specs=[any_] * 7,
            out_specs=pl.BlockSpec(memory_space=pltpu.VMEM),
            scratch_shapes=[
                pltpu.VMEM((2, top, tokens), jnp.int32),
                pltpu.VMEM((top, tokens), F32),
                pltpu.VMEM((8, top, tokens), jnp.int32),
                pltpu.VMEM((8, top, tokens), BF16),
                pltpu.VMEM((8, kn, tokens, kc), BF16),
                pltpu.VMEM((experts, 8 * slots, 2 * ff), F32),
                pltpu.VMEM((experts, 8 * slots, ff), BF16),
                pltpu.VMEM((experts, 8 * slots, kc), BF16),
                pltpu.VMEM((WR, 2, kc, ff), BF16),
                pltpu.VMEM((DR, ff, nc), BF16),
                pltpu.VMEM((8, rows, tokens), BF16),
                pltpu.VMEM((8, tokens, rows), BF16),
                pltpu.VMEM((nn, 4, tokens, nc), BF16),
                pltpu.VMEM((nn, 2, tokens, nc), BF16),
                pltpu.VMEM((nn, 2, half, nc), BF16),
                dma((2,)), dma((2,)),
                dma((6,)),
                dma,
                dma((4, kn)),
                dma((WR // GROUP,)), dma((DR // 4,)),
                dma((nn,)), dma((nn,)), dma((nn,)),
            ],
            compiler_params=pltpu.CompilerParams(
                collective_id=0, has_side_effects=True, vmem_limit_bytes=65_900_000
            ),
        )(expert, slot, gate, x, w_gate, w_up, w_down)
        return y[None, None]

    tok = P("dp", "ep", None, None)
    ws = P("ep", None, None)
    return jax.shard_map(
        local, mesh=mesh, in_specs=(tok, tok, tok, tok, ws, ws, ws), out_specs=tok, check_vma=False
    )
```

```python
import functools

import jax
import jax.numpy as jnp
from jax import lax
from jax.experimental import pallas as pl
from jax.experimental.pallas import tpu as pltpu
from jax.sharding import PartitionSpec as P

MESH = pl.DeviceIdType.MESH
F32, BF16 = jnp.float32, jnp.bfloat16

CORE, Y, X = 1, 2, 4
WR, DR = 12, 8
L2, L3 = 2, 5
GROUP = 4


def kernel(
    cfg, expert_ref, slot_ref, gate_ref, x_ref, wg_ref, wu_ref, wd_ref, o_ref,
    raw, rawg, codes, gates, xall, acc, hid, z, wring, dring, disp, comb, prec, r1, r2,
    meta_ss, meta_rs, load_s, send_s, ag_rs, wsem, dsem, p_rs, h1_rs, h2_rs,
):
    tokens, d, ff, experts, slots, kc, nc = cfg
    rows = experts * slots
    kn, nn = d // kc, d // nc
    half = tokens // 2
    wide = 2 * slots
    dp, me = lax.axis_index("dp"), lax.axis_index("ep")

    def dev(mask):
        to = me
        for bit in (CORE, Y, X):
            if mask & bit:
                to = to + bit - 2 * bit * ((me // bit) % 2)
        return (dp, to)

    def remote(src, dst, ss, rs, mask):
        return pltpu.make_async_remote_copy(
            src_ref=src, dst_ref=dst, send_sem=ss, recv_sem=rs, device_id=dev(mask), device_id_type=MESH
        )

    def landed(ref, sem):
        pltpu.make_async_copy(ref, ref, sem).wait()

    def w_start(first):
        for b in range(GROUP):
            i = first + b
            e, k, ring = i % experts, i // experts, i % WR
            at = pl.ds(pl.multiple_of(k * kc, kc), kc)
            sem = wsem.at[first // GROUP % (WR // GROUP)]
            pltpu.make_async_copy(wg_ref.at[e, at], wring.at[ring, 0], sem).start()
            pltpu.make_async_copy(wu_ref.at[e, at], wring.at[ring, 1], sem).start()

    def w_wait(first):
        landed(wring.at[pl.ds(first % WR, GROUP)], wsem.at[first // GROUP % (WR // GROUP)])

    def d_start(first):
        for b in range(4):
            i = first + b
            e, n, ring = i % experts, i // experts, i % DR
            at = pl.ds(pl.multiple_of(n * nc, nc), nc)
            pltpu.make_async_copy(wd_ref.at[e, :, at], dring.at[ring], dsem.at[first // 4 % (DR // 4)]).start()

    def d_wait(first):
        landed(dring.at[pl.ds(first % DR, 4)], dsem.at[first // 4 % (DR // 4)])

    top, low = pl.ds(0, half), pl.ds(half, half)

    def exchange(kind, src, dst, k, mask, at=None):
        src, dst = xall.at[src, k], xall.at[dst, k]
        if at is not None:
            src, dst = src.at[at], dst.at[at]
        return remote(src, dst, send_s, ag_rs.at[kind, k], mask)

    def first_x(k):
        return exchange(0, 0, X, k, X, top)

    def first_y(k):
        return exchange(0, 0, Y, k, Y, low)

    def second_x(k):
        return exchange(1, 0, X, k, X, low)

    def second_y(k):
        return exchange(1, 0, Y, k, Y, top)

    def to_core(k):
        return exchange(2, 0, CORE, k, CORE)

    def x_to_core(k):
        return exchange(2, X, X | CORE, k, CORE)

    def y_to_core(k):
        return exchange(2, Y, Y | CORE, k, CORE)

    def x_to_y(k):
        return exchange(3, X, X | Y, k, Y, top)

    def y_to_x(k):
        return exchange(3, Y, X | Y, k, X, low)

    def xy_to_core(k):
        return exchange(2, X | Y, 7, k, CORE)

    def own_start(k):
        at = pl.ds(pl.multiple_of(k * kc, kc), kc)
        pltpu.make_async_copy(x_ref.at[:, at], xall.at[0, k], load_s.at[3 + min(k, 2)]).start()

    loads = [
        pltpu.make_async_copy(expert_ref, raw.at[0], load_s.at[0]),
        pltpu.make_async_copy(slot_ref, raw.at[1], load_s.at[1]),
        pltpu.make_async_copy(gate_ref, rawg, load_s.at[2]),
    ]
    for copy in loads:
        copy.start()
    for k in range(2):
        own_start(k)
    barrier = pltpu.get_barrier_semaphore()
    for mask in range(1, 8):
        pl.semaphore_signal(barrier, inc=1, device_id=dev(mask), device_id_type=MESH)
    for copy in loads:
        copy.wait()
    codes[0] = jnp.where(raw[1] < slots, raw[0] * slots + raw[1], -1).astype(jnp.int16)
    gates[0] = rawg[...].astype(BF16)
    pl.semaphore_wait(barrier, 7)

    def send_codes(mask):
        return remote(codes.at[0], codes.at[mask], meta_ss.at[0], meta_rs.at[0], mask)

    def send_gates(mask):
        return remote(gates.at[0], gates.at[mask], meta_ss.at[1], meta_rs.at[1], mask)

    def send_first(k):
        first_x(k).start()
        first_y(k).start()

    def send_second(k):
        second_x(k).start()
        second_y(k).start()
        to_core(k).start()

    for mask in (6, 7, 4, 5, 2, 3, 1):
        send_codes(mask).start()
    landed(xall.at[0, 0], load_s.at[3])
    send_first(0)
    for mask in (6, 7, 4, 5, 2, 3, 1):
        send_gates(mask).start()
    send_second(0)
    landed(xall.at[0, 1], load_s.at[4])
    send_first(1)
    for k in range(2, kn):
        own_start(k)
    for i in range(0, WR, GROUP):
        w_start(i)

    def clear(e, _):
        acc[e] = jnp.zeros(acc.shape[1:], F32)
        return 0

    lax.fori_loop(0, experts, clear, 0)

    def table(r, values):
        row = lax.broadcasted_iota(jnp.int32, (rows, tokens), 0)
        code = codes[r].astype(jnp.int32) - me * rows
        out = jnp.zeros((rows, tokens), F32)
        for j in range(8):
            out = jnp.where(code[j : j + 1] == row, 1.0 if values is None else values[j : j + 1], out)
        return out

    def dispatch_table(r, _):
        disp[r] = table(r, None).astype(BF16)
        return 0

    def combine_table(r, _):
        comb[r] = jnp.transpose(table(r, gates[r].astype(F32))).astype(BF16)
        return 0

    landed(codes.at[pl.ds(1, 7)], meta_rs.at[0])
    lax.fori_loop(0, 8, dispatch_table, 0)

    def place(k):
        for pair in range(4):
            z0 = jnp.dot(disp[2 * pair], xall[2 * pair, k], preferred_element_type=F32)
            z1 = jnp.dot(disp[2 * pair + 1], xall[2 * pair + 1, k], preferred_element_type=F32)
            both = jnp.concatenate([z0.reshape(experts, slots, kc), z1.reshape(experts, slots, kc)], axis=1)
            z[:, pair * wide : (pair + 1) * wide, :] = both.astype(BF16)

    def project(k, run, last):
        first = k * experts + run * GROUP
        step = 256 if last else 512
        for b in range(GROUP):
            e, ring = run * GROUP + b, (first + b) % WR
            lhs = z[e]
            for c in range(0, ff, step):
                at, up = slice(c, c + step), slice(ff + c, ff + c + step)
                g = acc[e, :, at] + jnp.dot(lhs, wring[ring, 0, :, at], preferred_element_type=F32)
                u = acc[e, :, up] + jnp.dot(lhs, wring[ring, 1, :, at], preferred_element_type=F32)
                if last:
                    hid[e, :, at] = (g * lax.logistic(g) * u).astype(BF16)
                else:
                    acc[e, :, at] = g
                    acc[e, :, up] = u
        if not last:

            @pl.when(first + WR < experts * kn)
            def _():
                w_start(first + WR)

    def pass_first(k):
        landed(xall.at[0, k], ag_rs.at[0, k])
        x_to_y(k).start()
        y_to_x(k).start()

        @pl.when(k + 1 < kn)
        def _():
            send_second(k + 1)

    def pass_second(k):
        landed(xall.at[0, k], ag_rs.at[1, k])
        x_to_core(k).start()
        y_to_core(k).start()

        @pl.when(k + 2 < kn)
        def _():
            send_first(k + 2)

    def pass_across(k):
        landed(xall.at[X | Y, k], ag_rs.at[3, k])
        xy_to_core(k).start()

    def arrived(k):
        landed(xall.at[pl.ds(0, 4), k], ag_rs.at[2, k])

    def gather_step(t, _):
        pass_first(t)
        pass_across(t - 1)

        @pl.when(t >= 2)
        def _():
            w_wait((t - 2) * experts + GROUP)
            project(t - 2, 1, False)

        pass_second(t)
        w_wait((t - 1) * experts)
        arrived(t - 1)
        place(t - 1)
        project(t - 1, 0, False)
        return 0

    pass_first(0)
    landed(xall.at[0, pl.ds(2, kn - 2)], load_s.at[5])
    pass_second(0)
    landed(gates.at[pl.ds(1, 7)], meta_rs.at[1])
    lax.fori_loop(0, 8, combine_table, 0)
    lax.fori_loop(1, kn, gather_step, 0)
    pass_across(kn - 1)
    w_wait((kn - 2) * experts + GROUP)
    project(kn - 2, 1, False)
    for i in range(0, DR, 4):
        d_start(i)
    w_wait((kn - 1) * experts)
    w_wait((kn - 1) * experts + GROUP)
    arrived(kn - 1)
    place(kn - 1)
    for run in range(experts // GROUP):
        project(kn - 1, run, True)

    landed(xall.at[pl.ds(0, 7)], send_s)
    landed(codes.at[pl.ds(1, 7)], meta_ss.at[0])
    landed(gates.at[pl.ds(1, 7)], meta_ss.at[1])

    def to_part(n, q):
        return remote(xall.at[2 * q + 1, n], prec.at[n, q], send_s, p_rs.at[n], CORE)

    def hop1_x(n):
        return remote(xall.at[0, n], r1.at[n, 0], send_s, h1_rs.at[n], X)

    def hop1_y(n):
        return remote(xall.at[X, n], r1.at[n, 1], send_s, h1_rs.at[n], Y)

    def hop2_x(n):
        return remote(xall.at[Y, n, low], r2.at[n, 0], send_s, h2_rs.at[n], X)

    def hop2_y(n):
        return remote(xall.at[Y, n, top], r2.at[n, 1], send_s, h2_rs.at[n], Y)

    def col(q):
        return slice(q * nc, (q + 1) * nc)

    def last_projection(g, n):
        first = n * experts + 4 * g
        for a in range(2):
            got = [
                jnp.dot(
                    hid[4 * g + 2 * a + b], dring[(first + 2 * a + b) % DR], preferred_element_type=F32
                ).reshape(8, slots, nc)
                for b in range(2)
            ]
            both = jnp.concatenate(got, axis=1).astype(BF16)
            for b in range(2):
                z[4 * g + 2 * a + b] = both[4 * b : 4 * b + 4].reshape(8 * slots, nc)

        @pl.when(first + DR < experts * nn)
        def _():
            d_start(first + DR)

    def last_run(g, n):
        d_wait(n * experts + 4 * g)
        last_projection(g, n)

    def combine(n):
        def sums(r):
            at = slice(r % 4 * wide, (r % 4 + 1) * wide)
            mine = jnp.concatenate([z[2 * q + r // 4, at] for q in range(experts // 2)], axis=0)
            return jnp.dot(comb[r], mine, preferred_element_type=F32)

        for r in (7, 5, 3, 1):
            xall[r, n] = sums(r).astype(BF16)
        for r in (7, 5, 3, 1):
            to_part(n, r // 2).start()
        for r in (6, 4, 2, 0):
            acc[n, :tokens, col(r // 2)] = sums(r)

    def sum_cores(n):
        landed(prec.at[n], p_rs.at[n])
        for q in (3, 2, 1, 0):
            both = acc[n, :tokens, col(q)] + prec[n, q].astype(F32)
            acc[n, :tokens, col(q)] = both
            both = both.astype(BF16)
            if q == 3:
                xall[0, n, low] = both[:half]
                xall[X, n, low] = both[half:]
            if q == 2:
                xall[0, n, top] = both[:half]
                hop1_x(n).start()
            if q == 1:
                xall[X, n, top] = both[half:]
                hop1_y(n).start()

    def sum_first(n):
        landed(r1.at[n], h1_rs.at[n])
        xall[Y, n, top] = (acc[n, top, col(1)] + r1[n, 0, low].astype(F32)).astype(BF16)
        hop2_y(n).start()
        xall[Y, n, low] = (acc[n, low, col(2)] + r1[n, 1, low].astype(F32)).astype(BF16)
        hop2_x(n).start()

    def sum_second(n):
        at = pl.ds(pl.multiple_of(n * nc, nc), nc)
        landed(r2.at[n], h2_rs.at[n])
        o_ref[top, at] = (acc[n, top, col(0)] + r1[n, 0, top].astype(F32) + r2[n, 1].astype(F32)).astype(BF16)
        o_ref[low, at] = (acc[n, low, col(0)] + r1[n, 1, top].astype(F32) + r2[n, 0].astype(F32)).astype(BF16)

    stages = (
        (0, functools.partial(last_run, 0)), (1, sum_cores), (0, functools.partial(last_run, 1)),
        (0, combine), (L2, sum_first), (L3, sum_second),
    )

    def reduce_step(t, _):
        for lag, stage in stages:

            @pl.when((t >= lag) & (t < nn + lag))
            def _():
                stage(t - lag)

        return 0

    lax.fori_loop(0, nn + L3, reduce_step, 0)

    landed(xall.at[pl.ds(0, 7)], send_s)


def solution(mesh):
    def local(x, expert, slot, gate, w_gate, w_up, w_down):
        x = x.reshape(x.shape[-2:])
        tokens, d = x.shape
        top = expert.shape[-1]
        experts, _, ff = w_gate.shape
        total = experts * mesh.shape["ep"]
        slots = 5 * tokens * top // (4 * total)
        kc = nc = 256
        kn, nn = d // kc, d // nc
        rows, half = experts * slots, tokens // 2
        expert, slot, gate = (v.reshape(tokens, top).T for v in (expert, slot, gate))
        dma = pltpu.SemaphoreType.DMA
        any_ = pl.BlockSpec(memory_space=pl.ANY)
        y = pl.pallas_call(
            functools.partial(kernel, (tokens, d, ff, experts, slots, kc, nc)),
            out_shape=pltpu.VMEM((tokens, d), BF16),
            in_specs=[any_] * 7,
            out_specs=pl.BlockSpec(memory_space=pltpu.VMEM),
            scratch_shapes=[
                pltpu.VMEM((2, top, tokens), jnp.int32),
                pltpu.VMEM((top, tokens), F32),
                pltpu.VMEM((8, top, tokens), jnp.int16),
                pltpu.VMEM((8, top, tokens), BF16),
                pltpu.VMEM((8, kn, tokens, kc), BF16),
                pltpu.VMEM((experts, 8 * slots, 2 * ff), F32),
                pltpu.VMEM((experts, 8 * slots, ff), BF16),
                pltpu.VMEM((experts, 8 * slots, kc), BF16),
                pltpu.VMEM((WR, 2, kc, ff), BF16),
                pltpu.VMEM((DR, ff, nc), BF16),
                pltpu.VMEM((8, rows, tokens), BF16),
                pltpu.VMEM((8, tokens, rows), BF16),
                pltpu.VMEM((nn, 4, tokens, nc), BF16),
                pltpu.VMEM((nn, 2, tokens, nc), BF16),
                pltpu.VMEM((nn, 2, half, nc), BF16),
                dma((2,)), dma((2,)),
                dma((6,)),
                dma,
                dma((4, kn)),
                dma((WR // GROUP,)), dma((DR // 4,)),
                dma((nn,)), dma((nn,)), dma((nn,)),
            ],
            compiler_params=pltpu.CompilerParams(
                collective_id=0, has_side_effects=True, vmem_limit_bytes=65_900_000
            ),
        )(expert, slot, gate, x, w_gate, w_up, w_down)
        return y[None, None]

    tok = P("dp", "ep", None, None)
    ws = P("ep", None, None)
    return jax.shard_map(
        local, mesh=mesh, in_specs=(tok, tok, tok, tok, ws, ws, ws), out_specs=tok, check_vma=False
    )
```

```python
import functools

import jax
import jax.numpy as jnp
from jax import lax
from jax.experimental import pallas as pl
from jax.experimental.pallas import tpu as pltpu
from jax.sharding import PartitionSpec as P

MESH = pl.DeviceIdType.MESH
F32, BF16 = jnp.float32, jnp.bfloat16

CORE, Y, X = 1, 2, 4
WR, DR = 12, 8
L2, L3 = 2, 5
GROUP = 4


def kernel(
    cfg, expert_ref, slot_ref, gate_ref, x_ref, wg_ref, wu_ref, wd_ref, o_ref,
    raw, rawg, codes, gates, xall, acc, hid, z, wring, dring, disp, comb, prec, r1, r2,
    meta_ss, meta_rs, load_s, send_s, ag_rs, wsem, dsem, p_rs, h1_rs, h2_rs,
):
    tokens, d, ff, experts, slots, kc, nc = cfg
    rows = experts * slots
    kn, nn = d // kc, d // nc
    half = tokens // 2
    wide = 2 * slots
    dp, me = lax.axis_index("dp"), lax.axis_index("ep")

    def dev(mask):
        to = me
        for bit in (CORE, Y, X):
            if mask & bit:
                to = to + bit - 2 * bit * ((me // bit) % 2)
        return (dp, to)

    def remote(src, dst, ss, rs, mask):
        return pltpu.make_async_remote_copy(
            src_ref=src, dst_ref=dst, send_sem=ss, recv_sem=rs, device_id=dev(mask), device_id_type=MESH
        )

    def landed(ref, sem):
        pltpu.make_async_copy(ref, ref, sem).wait()

    def w_start(first):
        for b in range(GROUP):
            i = first + b
            e, k, ring = i % experts, i // experts, i % WR
            at = pl.ds(pl.multiple_of(k * kc, kc), kc)
            sem = wsem.at[first // GROUP % (WR // GROUP)]
            pltpu.make_async_copy(wg_ref.at[e, at], wring.at[ring, 0], sem).start()
            pltpu.make_async_copy(wu_ref.at[e, at], wring.at[ring, 1], sem).start()

    def w_wait(first):
        landed(wring.at[pl.ds(first % WR, GROUP)], wsem.at[first // GROUP % (WR // GROUP)])

    def d_start(first):
        for b in range(4):
            i = first + b
            e, n, ring = i % experts, i // experts, i % DR
            at = pl.ds(pl.multiple_of(n * nc, nc), nc)
            pltpu.make_async_copy(wd_ref.at[e, :, at], dring.at[ring], dsem.at[first // 4 % (DR // 4)]).start()

    def d_wait(first):
        landed(dring.at[pl.ds(first % DR, 4)], dsem.at[first // 4 % (DR // 4)])

    top, low = pl.ds(0, half), pl.ds(half, half)

    def exchange(kind, src, dst, k, mask, at=None):
        src, dst = xall.at[src, k], xall.at[dst, k]
        if at is not None:
            src, dst = src.at[at], dst.at[at]
        return remote(src, dst, send_s, ag_rs.at[kind, k], mask)

    def first_x(k):
        return exchange(0, 0, X, k, X, top)

    def first_y(k):
        return exchange(0, 0, Y, k, Y, low)

    def second_x(k):
        return exchange(1, 0, X, k, X, low)

    def second_y(k):
        return exchange(1, 0, Y, k, Y, top)

    def to_core(k):
        return exchange(2, 0, CORE, k, CORE)

    def x_to_core(k):
        return exchange(2, X, X | CORE, k, CORE)

    def y_to_core(k):
        return exchange(2, Y, Y | CORE, k, CORE)

    def x_to_y(k):
        return exchange(3, X, X | Y, k, Y, top)

    def y_to_x(k):
        return exchange(3, Y, X | Y, k, X, low)

    def xy_to_core(k):
        return exchange(2, X | Y, 7, k, CORE)

    def own_start(k):
        at = pl.ds(pl.multiple_of(k * kc, kc), kc)
        pltpu.make_async_copy(x_ref.at[:, at], xall.at[0, k], load_s.at[3 + min(k, 2)]).start()

    loads = [
        pltpu.make_async_copy(expert_ref, raw.at[0], load_s.at[0]),
        pltpu.make_async_copy(slot_ref, raw.at[1], load_s.at[1]),
        pltpu.make_async_copy(gate_ref, rawg, load_s.at[2]),
    ]
    for copy in loads:
        copy.start()
    for k in range(2):
        own_start(k)
    barrier = pltpu.get_barrier_semaphore()
    for mask in range(1, 8):
        pl.semaphore_signal(barrier, inc=1, device_id=dev(mask), device_id_type=MESH)
    for copy in loads:
        copy.wait()
    codes[0] = jnp.where(raw[1] < slots, raw[0] * slots + raw[1], -1).astype(jnp.int16)
    gates[0] = rawg[...].astype(BF16)
    pl.semaphore_wait(barrier, 7)

    def send_codes(mask):
        return remote(codes.at[0], codes.at[mask], meta_ss.at[0], meta_rs.at[0], mask)

    def send_gates(mask):
        return remote(gates.at[0], gates.at[mask], meta_ss.at[1], meta_rs.at[1], mask)

    def send_first(k):
        first_x(k).start()
        first_y(k).start()

    def send_second(k):
        second_x(k).start()
        second_y(k).start()
        to_core(k).start()

    for mask in (6, 7, 4, 5, 2, 3, 1):
        send_codes(mask).start()
    landed(xall.at[0, 0], load_s.at[3])
    send_first(0)
    for mask in (6, 7, 4, 5, 2, 3, 1):
        send_gates(mask).start()
    send_second(0)
    landed(xall.at[0, 1], load_s.at[4])
    send_first(1)
    for k in range(2, kn):
        own_start(k)
    for i in range(0, WR, GROUP):
        w_start(i)

    def clear(e, _):
        acc[e] = jnp.zeros(acc.shape[1:], F32)
        return 0

    lax.fori_loop(0, experts, clear, 0)

    def table(r, values):
        row = lax.broadcasted_iota(jnp.int32, (rows, tokens), 0)
        code = codes[r].astype(jnp.int32) - me * rows
        out = jnp.zeros((rows, tokens), F32)
        for j in range(8):
            out = jnp.where(code[j : j + 1] == row, 1.0 if values is None else values[j : j + 1], out)
        return out

    def dispatch_table(r, _):
        disp[r] = table(r, None).astype(BF16)
        return 0

    def combine_table(r, _):
        comb[r] = jnp.transpose(table(r, gates[r].astype(F32))).astype(BF16)
        return 0

    landed(codes.at[pl.ds(1, 7)], meta_rs.at[0])
    lax.fori_loop(0, 8, dispatch_table, 0)

    def place(k):
        for pair in range(4):
            z0 = jnp.dot(disp[2 * pair], xall[2 * pair, k], preferred_element_type=F32)
            z1 = jnp.dot(disp[2 * pair + 1], xall[2 * pair + 1, k], preferred_element_type=F32)
            both = jnp.concatenate([z0.reshape(experts, slots, kc), z1.reshape(experts, slots, kc)], axis=1)
            z[:, pair * wide : (pair + 1) * wide, :] = both.astype(BF16)

    def project(k, run, last):
        first = k * experts + run * GROUP
        step = 256 if last else 512
        for b in range(GROUP):
            e, ring = run * GROUP + b, (first + b) % WR
            lhs = z[e]
            for c in range(0, ff, step):
                at, up = slice(c, c + step), slice(ff + c, ff + c + step)
                g = acc[e, :, at] + jnp.dot(lhs, wring[ring, 0, :, at], preferred_element_type=F32)
                u = acc[e, :, up] + jnp.dot(lhs, wring[ring, 1, :, at], preferred_element_type=F32)
                if last:
                    hid[e, :, at] = (g * lax.logistic(g) * u).astype(BF16)
                else:
                    acc[e, :, at] = g
                    acc[e, :, up] = u
        if not last:

            @pl.when(first + WR < experts * kn)
            def _():
                w_start(first + WR)

    def pass_first(k):
        landed(xall.at[0, k], ag_rs.at[0, k])
        x_to_y(k).start()
        y_to_x(k).start()

        @pl.when(k + 1 < kn)
        def _():
            send_second(k + 1)

    def pass_second(k):
        landed(xall.at[0, k], ag_rs.at[1, k])
        x_to_core(k).start()
        y_to_core(k).start()

        @pl.when(k + 2 < kn)
        def _():
            send_first(k + 2)

    def pass_across(k):
        landed(xall.at[X | Y, k], ag_rs.at[3, k])
        xy_to_core(k).start()

    def arrived(k):
        landed(xall.at[pl.ds(0, 4), k], ag_rs.at[2, k])

    def gather_step(t, _):
        pass_first(t)
        pass_across(t - 1)

        @pl.when(t >= 2)
        def _():
            w_wait((t - 2) * experts + GROUP)
            project(t - 2, 1, False)

        pass_second(t)
        w_wait((t - 1) * experts)
        arrived(t - 1)
        place(t - 1)
        project(t - 1, 0, False)
        return 0

    pass_first(0)
    landed(xall.at[0, pl.ds(2, kn - 2)], load_s.at[5])
    pass_second(0)
    landed(gates.at[pl.ds(1, 7)], meta_rs.at[1])
    lax.fori_loop(0, 8, combine_table, 0)
    lax.fori_loop(1, kn, gather_step, 0)
    pass_across(kn - 1)
    w_wait((kn - 2) * experts + GROUP)
    project(kn - 2, 1, False)
    for i in range(0, DR, 4):
        d_start(i)
    w_wait((kn - 1) * experts)
    w_wait((kn - 1) * experts + GROUP)
    arrived(kn - 1)
    place(kn - 1)
    for run in range(experts // GROUP):
        project(kn - 1, run, True)

    landed(xall.at[pl.ds(0, 7)], send_s)
    landed(codes.at[pl.ds(1, 7)], meta_ss.at[0])
    landed(gates.at[pl.ds(1, 7)], meta_ss.at[1])

    def to_part(n, q):
        return remote(xall.at[2 * q + 1, n], prec.at[n, q], send_s, p_rs.at[n % 2], CORE)

    def hop1_x(n):
        return remote(xall.at[0, n], r1.at[n, 0], send_s, h1_rs.at[n], X)

    def hop1_y(n):
        return remote(xall.at[X, n], r1.at[n, 1], send_s, h1_rs.at[n], Y)

    def hop2_x(n):
        return remote(xall.at[Y, n, low], r2.at[n, 0], send_s, h2_rs.at[n], X)

    def hop2_y(n):
        return remote(xall.at[Y, n, top], r2.at[n, 1], send_s, h2_rs.at[n], Y)

    def col(q):
        return slice(q * nc, (q + 1) * nc)

    def last_projection(g, n):
        first = n * experts + 4 * g
        for a in range(2):
            got = [
                jnp.dot(
                    hid[4 * g + 2 * a + b], dring[(first + 2 * a + b) % DR], preferred_element_type=F32
                ).reshape(8, slots, nc)
                for b in range(2)
            ]
            both = jnp.concatenate(got, axis=1).astype(BF16)
            for b in range(2):
                z[4 * g + 2 * a + b] = both[4 * b : 4 * b + 4].reshape(8 * slots, nc)

        @pl.when(first + DR < experts * nn)
        def _():
            d_start(first + DR)

    def last_run(g, n):
        d_wait(n * experts + 4 * g)
        last_projection(g, n)

    def combine(n):
        def sums(r):
            at = slice(r % 4 * wide, (r % 4 + 1) * wide)
            mine = jnp.concatenate([z[2 * q + r // 4, at] for q in range(experts // 2)], axis=0)
            return jnp.dot(comb[r], mine, preferred_element_type=F32)

        for r in (7, 5, 3, 1):
            xall[r, n] = sums(r).astype(BF16)
        for r in (7, 5, 3, 1):
            to_part(n, r // 2).start()
        for r in (6, 4, 2, 0):
            acc[n, :tokens, col(r // 2)] = sums(r)

    def sum_cores(n):
        landed(prec.at[n], p_rs.at[n % 2])
        for q in (3, 1, 2, 0):
            both = acc[n, :tokens, col(q)] + prec[n, q].astype(F32)
            acc[n, :tokens, col(q)] = both
            both = both.astype(BF16)
            if q == 3:
                xall[0, n, low] = both[:half]
                xall[X, n, low] = both[half:]
            if q == 2:
                xall[0, n, top] = both[:half]
                hop1_x(n).start()
            if q == 1:
                xall[X, n, top] = both[half:]
                hop1_y(n).start()

    def sum_first(n):
        landed(r1.at[n], h1_rs.at[n])
        xall[Y, n, top] = (acc[n, top, col(1)] + r1[n, 0, low].astype(F32)).astype(BF16)
        hop2_y(n).start()
        xall[Y, n, low] = (acc[n, low, col(2)] + r1[n, 1, low].astype(F32)).astype(BF16)
        hop2_x(n).start()

    def sum_second(n):
        at = pl.ds(pl.multiple_of(n * nc, nc), nc)
        landed(r2.at[n], h2_rs.at[n])
        o_ref[top, at] = (acc[n, top, col(0)] + r1[n, 0, top].astype(F32) + r2[n, 1].astype(F32)).astype(BF16)
        o_ref[low, at] = (acc[n, low, col(0)] + r1[n, 1, top].astype(F32) + r2[n, 0].astype(F32)).astype(BF16)

    stages = (
        (0, functools.partial(last_run, 0)), (1, sum_cores), (0, functools.partial(last_run, 1)),
        (0, combine), (L2, sum_first), (L3, sum_second),
    )

    def reduce_step(t, _):
        for lag, stage in stages:

            @pl.when((t >= lag) & (t < nn + lag))
            def _():
                stage(t - lag)

        return 0

    lax.fori_loop(0, nn + L3, reduce_step, 0)

    landed(xall.at[pl.ds(0, 7)], send_s)


def solution(mesh):
    def local(x, expert, slot, gate, w_gate, w_up, w_down):
        x = x.reshape(x.shape[-2:])
        tokens, d = x.shape
        top = expert.shape[-1]
        experts, _, ff = w_gate.shape
        total = experts * mesh.shape["ep"]
        slots = 5 * tokens * top // (4 * total)
        kc = nc = 256
        kn, nn = d // kc, d // nc
        rows, half = experts * slots, tokens // 2
        expert, slot, gate = (v.reshape(tokens, top).T for v in (expert, slot, gate))
        dma = pltpu.SemaphoreType.DMA
        any_ = pl.BlockSpec(memory_space=pl.ANY)
        y = pl.pallas_call(
            functools.partial(kernel, (tokens, d, ff, experts, slots, kc, nc)),
            out_shape=pltpu.VMEM((tokens, d), BF16),
            in_specs=[any_] * 7,
            out_specs=pl.BlockSpec(memory_space=pltpu.VMEM),
            scratch_shapes=[
                pltpu.VMEM((2, top, tokens), jnp.int32),
                pltpu.VMEM((top, tokens), F32),
                pltpu.VMEM((8, top, tokens), jnp.int16),
                pltpu.VMEM((8, top, tokens), BF16),
                pltpu.VMEM((8, kn, tokens, kc), BF16),
                pltpu.VMEM((experts, 8 * slots, 2 * ff), F32),
                pltpu.VMEM((experts, 8 * slots, ff), BF16),
                pltpu.VMEM((experts, 8 * slots, kc), BF16),
                pltpu.VMEM((WR, 2, kc, ff), BF16),
                pltpu.VMEM((DR, ff, nc), BF16),
                pltpu.VMEM((8, rows, tokens), BF16),
                pltpu.VMEM((8, tokens, rows), BF16),
                pltpu.VMEM((nn, 4, tokens, nc), BF16),
                pltpu.VMEM((nn, 2, tokens, nc), BF16),
                pltpu.VMEM((nn, 2, half, nc), BF16),
                dma((2,)), dma((2,)),
                dma((6,)),
                dma,
                dma((4, kn)),
                dma((WR // GROUP,)), dma((DR // 4,)),
                dma((2,)), dma((nn,)), dma((nn,)),
            ],
            compiler_params=pltpu.CompilerParams(
                collective_id=0, has_side_effects=True, vmem_limit_bytes=65_900_000
            ),
        )(expert, slot, gate, x, w_gate, w_up, w_down)
        return y[None, None]

    tok = P("dp", "ep", None, None)
    ws = P("ep", None, None)
    return jax.shard_map(
        local, mesh=mesh, in_specs=(tok, tok, tok, tok, ws, ws, ws), out_specs=tok, check_vma=False
    )
```
